32 devices in a mesh: gx: 4 (over z), gy: 4 (over y, x), gz: 2 (over core).
Axes of the slice: x: 2, y: 2, z: 4, core: 2. Of those that a mesh axis runs over, the one named last changes fastest.
Arguments:
- cell_index: int32 [4, 4, 2, 8192], P('gx', 'gy', 'gz'), may hold values from 1431 to 167568, as said below
- offsets: float32 [4, 4, 2, 3, 8192], P('gx', 'gy', 'gz'), may hold values from -0.5 to 0.5
- mass: float32 [4, 4, 2, 8192], P('gx', 'gy', 'gz'), may hold values from 0.5 to 2
- counts: int32 [4, 4, 2], P('gx', 'gy', 'gz'), may hold values from 2048 to 8192, as said below
Outputs:
- density: float32 [512, 4, 8, 256], P(None, 'gx', 'gy', 'gz')
- spectrum: float32 [2, 256, 4, 8, 256], P(None, None, 'gx', 'gy', 'gz')
The draws below stay inside these ranges and needn't reach their ends.
Inputs may be any that keep to these rules, and one draw needn't show every extreme that they name: `cell_index`: each entry is (i + 1) * 10 * 130 + (j + 1) * 130 + k + 1 for a cell (i, j, k) with 0 <= i < 128, 0 <= j < 8, 0 <= k < 128; slots past a block's count hold such indices too. `counts`: some block is full in every draw.
All inputs are finite; a program needn't handle non-finite values.
Results may differ from the reference program's by a relative error of at most 0.0003.
Values sent between devices are 32-bit elements; how exact they have to be, the bound alone decides.
A program may use at most 64 MiB of HBM per device.

```python
import math
import jax
import jax.numpy as jnp
from jax import lax

CX = 128
YP = 2
CZ = 128
PCAP = 8192
CY = 8
NX = 512
NY = 32
NZ = 256
N_GX = 4
N_GY = 4
N_GZ = 2


def edge_biased(key, extent, full_shape):
    pick_key, place_key = jax.random.split(key)
    selector = jax.random.randint(pick_key, full_shape, 0, 8)
    spread = jax.random.randint(place_key, full_shape, 0, extent)
    return jnp.where(selector == 0, 0, jnp.where(selector == 1, extent - 1, spread)).astype(jnp.int32)


def draw_cell_index(key, part):
    full_shape = (N_GX, N_GY, N_GZ, PCAP)
    key_list = jax.random.split(jax.random.fold_in(key, 11), 3)
    coord_x = edge_biased(key_list[0], CX, full_shape)
    coord_y = edge_biased(key_list[1], CY, full_shape)
    coord_z = edge_biased(key_list[2], CZ, full_shape)
    return (((coord_x + 1) * (CY + 2) + coord_y + 1) * (CZ + 2) + coord_z + 1).astype(jnp.int32)


def draw_counts(key, part):
    full_shape = (N_GX, N_GY, N_GZ)
    key_list = jax.random.split(jax.random.fold_in(key, 23), 3)
    base_load = jax.random.randint(key_list[0], full_shape, PCAP // 4, PCAP // 2 + 1)
    heavy = jax.random.randint(key_list[1], full_shape, 0, 16) == 0
    loads = jnp.where(heavy, PCAP, base_load).reshape(-1)
    fullest = jax.random.randint(key_list[2], (), 0, N_GX * N_GY * N_GZ)
    loads = loads.at[fullest].set(PCAP)
    return loads.reshape(full_shape).astype(jnp.int32)


def shard_levels(rng, dims, shards, low, high):
    def one(axis_at, parts):
        steps = jax.random.uniform(jax.random.fold_in(jax.random.fold_in(rng, 6), axis_at), (parts,), jnp.float32, low / len(shards), high / len(shards))
        return jnp.repeat(jnp.exp(steps), dims[axis_at] // parts).reshape((-1,) + (1,) * (len(dims) - axis_at - 1))

    loudness = one(*shards[0])
    for cut in shards[1:]:
        loudness = loudness * one(*cut)
    return loudness


def setup_inputs(seed: int = 0) -> dict:
    keys = jax.random.split(jax.random.key(seed), 5)
    cell_index = draw_cell_index(jax.random.fold_in(keys[4], 71), 0)
    offsets = jnp.clip(jax.random.uniform(keys[1], (N_GX, N_GY, N_GZ, 3, PCAP), jnp.float32, -0.5, 0.5) * shard_levels(keys[1], (N_GX, N_GY, N_GZ, 3, PCAP), ((0, 4), (1, 4), (2, 2)), -0.4, 0.0), -0.5, 0.5)
    mass = jnp.clip(jnp.exp(math.log(2.0) - 1.3862944 * jax.random.uniform(keys[2], (N_GX, N_GY, N_GZ, PCAP), jnp.float32) ** shard_levels(keys[2], (N_GX, N_GY, N_GZ, PCAP), ((0, 4), (1, 4), (2, 2)), -0.2, 0.2)), 0.5, 2.0)
    counts = draw_counts(jax.random.fold_in(keys[4], 71), 0)
    return {"cell_index": cell_index, "offsets": offsets, "mass": mass, "counts": counts}


def to_pencils(field):
    leading = field.shape[:-3]
    split = field.reshape(leading + (field.shape[-3], N_GY, N_GX, YP, NZ))
    moved = jnp.moveaxis(split, -4, -3)
    return moved.reshape(leading + (field.shape[-3], N_GX, N_GY * YP, NZ))

def reference(cell_index, offsets, mass, counts):
    full_shape = (N_GX, N_GY, N_GZ, PCAP)
    plane = (CY + 2) * (CZ + 2)
    block_x = lax.broadcasted_iota(jnp.int32, full_shape, 0)
    block_y = lax.broadcasted_iota(jnp.int32, full_shape, 1)
    block_z = lax.broadcasted_iota(jnp.int32, full_shape, 2)
    slot_ids = lax.broadcasted_iota(jnp.int32, full_shape, 3)
    pos_x = cell_index // plane - 1 + block_x * CX
    pos_y = cell_index // (CZ + 2) % (CY + 2) - 1 + block_y * CY
    pos_z = cell_index % (CZ + 2) - 1 + block_z * CZ
    loaded = jnp.where(slot_ids < counts[..., None], mass, jnp.float32(0.0))
    positions = (pos_x, pos_y, pos_z)
    extents = (NX, NY, NZ)
    shifts = [offsets[:, :, :, axis_pos, :] for axis_pos in range(3)]
    signs = [jnp.where(shifts[axis_pos] >= 0.0, 1, -1).astype(jnp.int32) for axis_pos in range(3)]
    field = jnp.zeros((NX * NY * NZ,), jnp.float32)
    for corner in range(8):
        factor = None
        targets = []
        for axis_pos in range(3):
            upper_bit = corner >> 2 - axis_pos & 1
            magnitude = jnp.abs(shifts[axis_pos])
            if upper_bit:
                target = (positions[axis_pos] + signs[axis_pos]) % extents[axis_pos]
                factor_one = magnitude
            else:
                target = positions[axis_pos] % extents[axis_pos]
                factor_one = 1.0 - magnitude
            targets.append(target.astype(jnp.int32))
            factor = factor_one if factor is None else factor * factor_one
        weight = factor * loaded
        flat_cell = ((targets[0] * NY + targets[1]) * NZ + targets[2]).astype(jnp.int32)
        field = field.at[flat_cell.reshape(-1)].add(weight.reshape(-1))
    field = field.reshape(NX, NY, NZ)
    modes = jnp.fft.rfft(field, axis=0)[:NX // 2]
    scale = 1.0 / math.sqrt(NX)
    spectrum = jnp.stack([jnp.real(modes), jnp.imag(modes)]).astype(jnp.float32) * scale
    return (to_pencils(field), to_pencils(spectrum))
```

```python
import functools
import math

import jax
import jax.numpy as jnp
from jax import lax
from jax.experimental import pallas as pl
from jax.experimental.pallas import tpu as pltpu
from jax.sharding import PartitionSpec as P

CX = 128
YP = 2
CZ = 128


def up(n, m):
    return -(-n // m) * m


def split(value):
    high = value.astype(jnp.bfloat16)
    low = (value - high.astype(jnp.float32)).astype(jnp.bfloat16)
    return high, low


def nt_dot(lhs, rhs):
    return lax.dot_general(lhs, rhs, (((1,), (1,)), ((), ())), preferred_element_type=jnp.float32)


def paint_kernel(rows_y, chunk, live_ref, cell_ref, off_ref, mass_ref, core_ref, xg_ref, zg_ref, cg_ref, acc, accx, accz, corner, lhs, near, far):
    padded_y = rows_y + 2
    band = up(padded_y, 8)
    stride_y = CZ + 2
    stride_x = padded_y * stride_y
    total = cell_ref.shape[1]
    live = live_ref[0]
    acc[...] = jnp.zeros_like(acc)
    accx[...] = jnp.zeros_like(accx)
    accz[...] = jnp.zeros_like(accz)
    corner[...] = jnp.zeros_like(corner)
    row_core = lax.broadcasted_iota(jnp.int32, (CX, chunk), 0).astype(jnp.float32) + 1.0
    row_band = lax.broadcasted_iota(jnp.int32, (2 * band, chunk), 0).astype(jnp.float32)

    def step(turn, carry):
        start = pl.multiple_of(turn * chunk, chunk)
        here = pl.ds(start, chunk)
        slot = start + lax.broadcasted_iota(jnp.int32, (1, chunk), 1)
        loaded = jnp.where(slot < live, mass_ref[:, here], 0.0)
        cell = cell_ref[:, here].astype(jnp.float32)
        x0 = jnp.floor((cell + 0.5) * (1.0 / stride_x))
        rest = cell - x0 * stride_x
        y0 = jnp.floor((rest + 0.5) * (1.0 / stride_y))
        z0 = rest - y0 * stride_y
        dx = off_ref[0:1, here]
        dy = off_ref[1:2, here]
        dz = off_ref[2:3, here]
        x1 = x0 + jnp.where(dx >= 0.0, 1.0, -1.0)
        y1 = y0 + jnp.where(dy >= 0.0, 1.0, -1.0)
        z1 = z0 + jnp.where(dz >= 0.0, 1.0, -1.0)
        fx, fy, fz = jnp.abs(dx), jnp.abs(dy), jnp.abs(dz)
        ex, ey, ez = 1.0 - fx, 1.0 - fy, 1.0 - fz
        my0, my1 = ey * loaded, fy * loaded
        zhot = jnp.where(row_core == z0, ez, jnp.where(row_core == z1, fz, 0.0))
        zhi, zlo = split(zhot)
        zrhs = jnp.concatenate([zhi, zlo], axis=0)
        xhot = jnp.where(row_core == x0, ex, jnp.where(row_core == x1, fx, 0.0))
        xhi, xlo = split(xhot)
        xrhs = jnp.concatenate([xhi, xlo], axis=0)
        near[...] = xhot * my0
        far[...] = xhot * my1
        yhot = jnp.where(row_band == y0, my0, jnp.where(row_band == y1, my1, 0.0)) + jnp.where(
            row_band == y0 + band, my0, jnp.where(row_band == y1 + band, my1, 0.0)
        )
        side = jnp.where(row_band >= band, 1.0, 0.0)
        ghost_x = jnp.where(x1 == side * (CX + 1.0), fx, 0.0) * yhot
        ghost_z = jnp.where(z1 == side * (CZ + 1.0), fz, 0.0) * yhot
        gxh, gxl = split(ghost_x)
        accx[...] += nt_dot(jnp.concatenate([gxh, gxl], axis=0), zrhs)
        gzh, gzl = split(ghost_z)
        accz[...] += nt_dot(jnp.concatenate([gzh, gzl], axis=0), xrhs)
        for which, edge in enumerate((0.0, CX + 1.0)):
            part = ghost_z * jnp.where(x1 == edge, fx, 0.0)
            for piece in range(chunk // 128):
                corner[which] += part[:, piece * 128 : (piece + 1) * 128]
        for y in range(padded_y):
            value = jnp.where(y0 == float(y), near[...], jnp.where(y1 == float(y), far[...], 0.0))
            high, low = split(value)
            lhs[y, :CX] = high
            lhs[y, CX:] = low
            acc[y] += nt_dot(lhs[y], zrhs)
        return carry

    turns = lax.div(live + (chunk - 1), chunk)
    lax.fori_loop(0, turns, step, 0)

    def gather(ref, rows):
        full = ref[...]
        return (full[:rows, :128] + full[rows:, :128]) + (full[:rows, 128:] + full[rows:, 128:])

    for y in range(padded_y):
        core_ref[y] = gather(acc.at[y], CX)
    xg_ref[...] = gather(accx, 2 * band)
    zg_ref[...] = gather(accz, 2 * band)
    lane = lax.broadcasted_iota(jnp.int32, (2 * band, 128), 1)
    low = jnp.sum(corner[0], axis=1, keepdims=True)
    high = jnp.sum(corner[1], axis=1, keepdims=True)
    cg_ref[...] = jnp.where(lane == 0, low, jnp.where(lane == 1, high, 0.0))


def paint(cell, offs, mass, live, rows_y):
    total = cell.shape[1]
    chunk = math.gcd(1024, total)
    band = up(rows_y + 2, 8)
    padded_y = rows_y + 2
    vmem = pl.BlockSpec(memory_space=pltpu.VMEM)
    return pl.pallas_call(
        functools.partial(paint_kernel, rows_y, chunk),
        out_shape=[
            jax.ShapeDtypeStruct((padded_y, CX, CZ), jnp.float32),
            jax.ShapeDtypeStruct((2 * band, CZ), jnp.float32),
            jax.ShapeDtypeStruct((2 * band, CX), jnp.float32),
            jax.ShapeDtypeStruct((2 * band, 128), jnp.float32),
        ],
        in_specs=[pl.BlockSpec(memory_space=pltpu.SMEM), vmem, vmem, vmem],
        out_specs=[vmem] * 4,
        scratch_shapes=[
            pltpu.VMEM((padded_y, 2 * CX, 256), jnp.float32),
            pltpu.VMEM((4 * band, 256), jnp.float32),
            pltpu.VMEM((4 * band, 256), jnp.float32),
            pltpu.VMEM((2, 2 * band, 128), jnp.float32),
            pltpu.VMEM((padded_y, 2 * CX, chunk), jnp.bfloat16),
            pltpu.VMEM((CX, chunk), jnp.float32),
            pltpu.VMEM((CX, chunk), jnp.float32),
        ],
    )(live, cell, offs, mass)


def with_halo(cells, sides, width):
    for axis, dim in sides:
        count = lax.axis_size(axis)
        head = lax.slice_in_dim(cells, 0, width, axis=dim)
        tail = lax.slice_in_dim(cells, cells.shape[dim] - width, cells.shape[dim], axis=dim)
        cells = jnp.concatenate(
            [
                lax.ppermute(tail, axis, [(i, (i + 1) % count) for i in range(count)]),
                cells,
                lax.ppermute(head, axis, [((i + 1) % count, i) for i in range(count)]),
            ],
            axis=dim,
        )
    return cells


def collapse(extended, axis_dim):
    inner_len = extended.shape[axis_dim] - 4
    core_part = lax.slice_in_dim(extended, 2, inner_len + 2, axis=axis_dim)
    low_ghost = lax.slice_in_dim(extended, 0, 1, axis=axis_dim)
    high_ghost = lax.slice_in_dim(extended, inner_len + 3, inner_len + 4, axis=axis_dim)
    first_row = lax.slice_in_dim(core_part, 0, 1, axis=axis_dim) + low_ghost
    middle = lax.slice_in_dim(core_part, 1, inner_len - 1, axis=axis_dim)
    last_row = lax.slice_in_dim(core_part, inner_len - 1, inner_len, axis=axis_dim) + high_ghost
    return jnp.concatenate([first_row, middle, last_row], axis=axis_dim)


def dft_tables(count_out, count_in, period):
    rows_out = lax.iota(jnp.int32, count_out)
    rows_in = lax.iota(jnp.int32, count_in)
    phase = (rows_out[:, None] * rows_in[None, :] % period).astype(jnp.float32)
    angle = phase * jnp.float32(2.0 * math.pi / period)
    return (jnp.cos(angle), jnp.sin(angle))


def body(cell_index, offsets, mass, counts):
    groups = lax.axis_size("gx")
    width_y = YP * groups
    depth_z = CZ
    core, xg, zg, cg = paint(
        cell_index.reshape(1, -1), offsets.reshape(3, -1), mass.reshape(1, -1), counts.reshape(1), width_y
    )
    padded_y = width_y + 2
    band = up(padded_y, 8)
    inner = jnp.moveaxis(core, 0, 1)
    edges = [xg[side * band : side * band + padded_y] for side in range(2)]
    full_x = jnp.concatenate([edges[0][None], inner, edges[1][None]], axis=0)
    walls = []
    for side in range(2):
        rows = slice(side * band, side * band + padded_y)
        wall = jnp.concatenate([cg[rows, 0:1], zg[rows], cg[rows, 1:2]], axis=1)
        walls.append(jnp.swapaxes(wall, 0, 1)[:, :, None])
    block = jnp.concatenate([walls[0], full_x, walls[1]], axis=2)
    extended = with_halo(block, (("gy", 1), ("gz", 2)), 1)
    folded = collapse(collapse(extended, 1), 2)
    pencil = lax.all_to_all(folded, "gx", split_axis=1, concat_axis=0, tiled=True)
    stacked = pencil.reshape(groups, CX + 2, YP, depth_z)
    core_part = stacked[:, 1 : CX + 1]
    low_ghost = jnp.roll(stacked[:, 0], -1, axis=0)
    high_ghost = jnp.roll(stacked[:, CX + 1], 1, axis=0)
    core_part = core_part.at[:, 0].add(high_ghost).at[:, CX - 1].add(low_ghost)
    density = core_part.reshape(groups * CX, YP, depth_z)
    length = groups * CX
    power = length.bit_length() - 1
    split_b = 2 ** (power // 2)
    split_a = length // split_b
    highest = lax.Precision.HIGHEST
    cos_b, sin_b = dft_tables(split_b, split_b, split_b)
    columns = density.reshape(split_b, split_a, YP * depth_z)
    first_real = jnp.einsum("kb,bar->kar", cos_b, columns, precision=highest)
    first_imag = -jnp.einsum("kb,bar->kar", sin_b, columns, precision=highest)
    twist_cos, twist_sin = dft_tables(split_b, split_a, length)
    twist_cos = twist_cos[:, :, None]
    twist_sin = twist_sin[:, :, None]
    turned_real = first_real * twist_cos + first_imag * twist_sin
    turned_imag = first_imag * twist_cos - first_real * twist_sin
    cos_a, sin_a = dft_tables(split_a // 2, split_a, split_a)
    final_real = jnp.einsum("ja,kar->jkr", cos_a, turned_real, precision=highest) + jnp.einsum(
        "ja,kar->jkr", sin_a, turned_imag, precision=highest
    )
    final_imag = jnp.einsum("ja,kar->jkr", cos_a, turned_imag, precision=highest) - jnp.einsum(
        "ja,kar->jkr", sin_a, turned_real, precision=highest
    )
    scale = 1.0 / math.sqrt(length)
    spectrum = jnp.stack([final_real, final_imag]) * scale
    spectrum = spectrum.reshape(2, length // 2, 1, YP, depth_z)
    return (density.reshape(length, 1, YP, depth_z), spectrum)


def solution(mesh):
    placed = (
        P("gx", "gy", "gz", None),
        P("gx", "gy", "gz", None, None),
        P("gx", "gy", "gz", None),
        P("gx", "gy", "gz"),
    )
    return jax.shard_map(
        body,
        mesh=mesh,
        in_specs=placed,
        out_specs=(P(None, "gx", "gy", "gz"), P(None, None, "gx", "gy", "gz")),
        check_vma=False,
    )
```

```python
import functools
import math

import jax
import jax.numpy as jnp
import numpy as np
from jax import lax
from jax.experimental import pallas as pl
from jax.experimental.pallas import tpu as pltpu
from jax.sharding import PartitionSpec as P

MESH = pl.DeviceIdType.MESH
CX = 128
YP = 2
CZ = 128


def up(n, m):
    return -(-n // m) * m


def split(value):
    high = value.astype(jnp.bfloat16)
    low = (value - high.astype(jnp.float32)).astype(jnp.bfloat16)
    return high, low


def nt_dot(lhs, rhs):
    return lax.dot_general(lhs, rhs, (((1,), (1,)), ((), ())), preferred_element_type=jnp.float32)


def paint_kernel(rows_y, chunk, live_ref, cell_ref, off_ref, mass_ref, core_ref, xg_ref, zg_ref, acc, accx, accz, corner, lhs, near, far):
    padded_y = rows_y + 2
    band = up(padded_y, 8)
    stride_y = CZ + 2
    stride_x = padded_y * stride_y
    total = cell_ref.shape[1]
    live = live_ref[0]
    acc[...] = jnp.zeros_like(acc)
    accx[...] = jnp.zeros_like(accx)
    accz[...] = jnp.zeros_like(accz)
    corner[...] = jnp.zeros_like(corner)
    row_core = lax.broadcasted_iota(jnp.int32, (CX, chunk), 0).astype(jnp.float32) + 1.0
    row_band = lax.broadcasted_iota(jnp.int32, (2 * band, chunk), 0).astype(jnp.float32)

    def step(turn, carry):
        start = pl.multiple_of(turn * chunk, chunk)
        here = pl.ds(start, chunk)
        slot = start + lax.broadcasted_iota(jnp.int32, (1, chunk), 1)
        loaded = jnp.where(slot < live, mass_ref[:, here], 0.0)
        cell = cell_ref[:, here].astype(jnp.float32)
        x0 = jnp.floor((cell + 0.5) * (1.0 / stride_x))
        rest = cell - x0 * stride_x
        y0 = jnp.floor((rest + 0.5) * (1.0 / stride_y))
        z0 = rest - y0 * stride_y
        dx = off_ref[0:1, here]
        dy = off_ref[1:2, here]
        dz = off_ref[2:3, here]
        x1 = x0 + jnp.where(dx >= 0.0, 1.0, -1.0)
        y1 = y0 + jnp.where(dy >= 0.0, 1.0, -1.0)
        z1 = z0 + jnp.where(dz >= 0.0, 1.0, -1.0)
        fx, fy, fz = jnp.abs(dx), jnp.abs(dy), jnp.abs(dz)
        ex, ey, ez = 1.0 - fx, 1.0 - fy, 1.0 - fz
        my0, my1 = ey * loaded, fy * loaded
        zhot = jnp.where(row_core == z0, ez, jnp.where(row_core == z1, fz, 0.0))
        zhi, zlo = split(zhot)
        zrhs = jnp.concatenate([zhi, zlo], axis=0)
        xhot = jnp.where(row_core == x0, ex, jnp.where(row_core == x1, fx, 0.0))
        xhi, xlo = split(xhot)
        xrhs = jnp.concatenate([xhi, xlo], axis=0)
        near[...] = xhot * my0
        far[...] = xhot * my1
        yhot = jnp.where(row_band == y0, my0, jnp.where(row_band == y1, my1, 0.0)) + jnp.where(
            row_band == y0 + band, my0, jnp.where(row_band == y1 + band, my1, 0.0)
        )
        side = jnp.where(row_band >= band, 1.0, 0.0)
        ghost_x = jnp.where(x1 == side * (CX + 1.0), fx, 0.0) * yhot
        ghost_z = jnp.where(z1 == side * (CZ + 1.0), fz, 0.0) * yhot
        gxh, gxl = split(ghost_x)
        accx[...] += nt_dot(jnp.concatenate([gxh, gxl], axis=0), zrhs)
        gzh, gzl = split(ghost_z)
        accz[...] += nt_dot(jnp.concatenate([gzh, gzl], axis=0), xrhs)
        for which, edge in enumerate((0.0, CX + 1.0)):
            part = ghost_z * jnp.where(x1 == edge, fx, 0.0)
            for piece in range(chunk // 128):
                corner[which] += part[:, piece * 128 : (piece + 1) * 128]
        for y in range(padded_y):
            value = jnp.where(y0 == float(y), near[...], jnp.where(y1 == float(y), far[...], 0.0))
            high, low = split(value)
            lhs[y, :CX] = high
            lhs[y, CX:] = low
            acc[y] += nt_dot(lhs[y], zrhs)
        return carry

    turns = lax.div(live + (chunk - 1), chunk)
    lax.fori_loop(0, turns, step, 0)

    def gather(ref, rows):
        full = ref[...]
        return (full[:rows, :128] + full[rows:, :128]) + (full[:rows, 128:] + full[rows:, 128:])

    for y in range(padded_y):
        core_ref[y] = gather(acc.at[y], CX)
    xg_ref[...] = gather(accx, 2 * band)
    zg_ref[:, :CX] = gather(accz, 2 * band)
    lane = lax.broadcasted_iota(jnp.int32, (2 * band, 128), 1)
    low = jnp.sum(corner[0], axis=1, keepdims=True)
    high = jnp.sum(corner[1], axis=1, keepdims=True)
    zg_ref[:, CX:] = jnp.where(lane == 0, low, jnp.where(lane == 1, high, 0.0))


def paint(cell, offs, mass, live, rows_y):
    total = cell.shape[1]
    chunk = math.gcd(1024, total)
    band = up(rows_y + 2, 8)
    padded_y = rows_y + 2
    vmem = pl.BlockSpec(memory_space=pltpu.VMEM)
    return pl.pallas_call(
        functools.partial(paint_kernel, rows_y, chunk),
        out_shape=[
            jax.ShapeDtypeStruct((padded_y, CX, CZ), jnp.float32),
            jax.ShapeDtypeStruct((2 * band, CZ), jnp.float32),
            jax.ShapeDtypeStruct((2 * band, 2 * CX), jnp.float32),
        ],
        in_specs=[pl.BlockSpec(memory_space=pltpu.SMEM), vmem, vmem, vmem],
        out_specs=[vmem] * 3,
        scratch_shapes=[
            pltpu.VMEM((padded_y, 2 * CX, 256), jnp.float32),
            pltpu.VMEM((4 * band, 256), jnp.float32),
            pltpu.VMEM((4 * band, 256), jnp.float32),
            pltpu.VMEM((2, 2 * band, 128), jnp.float32),
            pltpu.VMEM((padded_y, 2 * CX, chunk), jnp.bfloat16),
            pltpu.VMEM((CX, chunk), jnp.float32),
            pltpu.VMEM((CX, chunk), jnp.float32),
        ],
    )(live, cell, offs, mass)


ROWS = CX + 8


def exchange_kernel(dims, rows_y, core_ref, xg_ref, zg_ref, fhi_hbm, flo_hbm, dens_ref, spec_ref, zin, yout, yin, pen, inbox, flat, fhi, flo, table_sem, z_send, z_recv, y_send, y_recv, x_send, x_recv):
    groups, count_y, count_z = dims
    padded_y = rows_y + 2
    band = up(padded_y, 8)
    length = groups * CX
    gx, gy, gz = lax.axis_index("gx"), lax.axis_index("gy"), lax.axis_index("gz")
    y_next = (lax.rem(gy + count_y - 1, count_y), lax.rem(gy + 1, count_y))
    z_next = (lax.rem(gz + count_z - 1, count_z), lax.rem(gz + 1, count_z))
    tables = [
        pltpu.make_async_copy(fhi_hbm, fhi, table_sem.at[0]),
        pltpu.make_async_copy(flo_hbm, flo, table_sem.at[1]),
    ]
    for table in tables:
        table.start()
    barrier = pltpu.get_barrier_semaphore()
    for other in z_next:
        pl.semaphore_signal(barrier, inc=1, device_id={"gz": other}, device_id_type=MESH)
    for other in y_next:
        pl.semaphore_signal(barrier, inc=1, device_id={"gy": other}, device_id_type=MESH)
    for step in range(1, groups):
        pl.semaphore_signal(barrier, inc=1, device_id={"gx": lax.rem(gx + step, groups)}, device_id_type=MESH)
    pl.semaphore_wait(barrier, groups + 3)

    z_copies = [
        pltpu.make_async_remote_copy(
            src_ref=zg_ref.at[pl.ds(side * band, band)],
            dst_ref=zin.at[side],
            send_sem=z_send.at[side],
            recv_sem=z_recv.at[side],
            device_id={"gz": z_next[side]},
            device_id_type=MESH,
        )
        for side in range(2)
    ]
    for copy in z_copies:
        copy.start()
    for copy in z_copies:
        copy.wait()
    lane = lax.broadcasted_iota(jnp.int32, (CX, CZ), 1)
    ends = (lane == CZ - 1, lane == 0)
    columns = [zin[side].T for side in range(2)]
    edge_lane = lax.broadcasted_iota(jnp.int32, (band, CZ), 1)
    edges = []
    for x_side in range(2):
        edge = xg_ref[x_side * band : (x_side + 1) * band]
        edge = edge + jnp.where(edge_lane == CZ - 1, zin[0][:, CX + x_side : CX + x_side + 1], 0.0)
        edge = edge + jnp.where(edge_lane == 0, zin[1][:, CX + x_side : CX + x_side + 1], 0.0)
        edges.append(edge)

    def fold(target, index):
        whole = core_ref[index]
        for side in range(2):
            whole = whole + jnp.where(ends[side], columns[side][:CX, index : index + 1], 0.0)
        target[:CX] = whole
        target[CX:] = jnp.concatenate(
            [edges[0][index : index + 1], edges[1][index : index + 1], jnp.zeros((6, CZ), jnp.float32)], axis=0
        )

    fold(yout.at[0], 0)
    fold(yout.at[1], padded_y - 1)
    y_copies = [
        pltpu.make_async_remote_copy(
            src_ref=yout.at[side],
            dst_ref=yin.at[side],
            send_sem=y_send.at[side],
            recv_sem=y_recv.at[side],
            device_id={"gy": y_next[side]},
            device_id_type=MESH,
        )
        for side in range(2)
    ]
    for copy in y_copies:
        copy.start()

    def pencil_copy(target):
        return pltpu.make_async_remote_copy(
            src_ref=pen.at[target],
            dst_ref=inbox.at[gx],
            send_sem=x_send.at[target],
            recv_sem=x_recv.at[gx],
            device_id={"gx": target},
            device_id_type=MESH,
        )

    def ship(target):
        @pl.when(gx != target)
        def _():
            pencil_copy(target).start()

    middle = list(range(1, groups - 1))
    for target in middle:
        for row in range(YP):
            fold(pen.at[target, row], 1 + target * YP + row)
        ship(target)
    for target in (0, groups - 1):
        for row in range(YP):
            fold(pen.at[target, row], 1 + target * YP + row)
    for copy in y_copies:
        copy.wait()
    pen[groups - 1, YP - 1] += yin[0]
    pen[0, 0] += yin[1]
    ship(0)
    ship(groups - 1)
    inbox[gx] = pen[gx]
    for source in range(groups):
        @pl.when(gx != source)
        def _():
            pencil_copy(source).wait_send()
            pltpu.make_async_remote_copy(
                src_ref=pen.at[source],
                dst_ref=inbox.at[source],
                send_sem=x_send.at[source],
                recv_sem=x_recv.at[source],
                device_id={"gx": source},
                device_id_type=MESH,
            ).wait_recv()

    row_id = lax.broadcasted_iota(jnp.int32, (CX, CZ), 0)
    for block in range(groups):
        before, after = (block - 1) % groups, (block + 1) % groups
        for row in range(YP):
            value = inbox[block, row, :CX]
            value = value + jnp.where(row_id == 0, inbox[before, row, CX + 1 : CX + 2], 0.0)
            value = value + jnp.where(row_id == CX - 1, inbox[after, row, CX : CX + 1], 0.0)
            dens_ref[pl.ds(block * CX * YP + row, CX, stride=YP), :] = value
            high, low = split(value)
            flat[0, pl.ds(block * CX, CX), pl.ds(row * CZ, CZ)] = high
            flat[1, pl.ds(block * CX, CX), pl.ds(row * CZ, CZ)] = low
    for table in tables:
        table.wait()
    tile = 128

    def transform(turn, carry):
        start = pl.multiple_of(turn * tile, tile)
        rows = pl.ds(start, tile)
        both = jnp.dot(fhi[rows, :], flat[0], preferred_element_type=jnp.float32)
        both += jnp.dot(flo[rows, :], flat[0], preferred_element_type=jnp.float32)
        both += jnp.dot(fhi[rows, :], flat[1], preferred_element_type=jnp.float32)
        for row in range(YP):
            spec_ref[pl.ds(start * YP + row, tile, stride=YP), :] = both[:, row * CZ : (row + 1) * CZ]
        return carry

    lax.fori_loop(0, length // tile, transform, 0)


def exchange(dims, rows_y, core, xg, zg):
    groups = dims[0]
    length = groups * CX
    half = length // 2
    band = up(rows_y + 2, 8)
    angle = (np.arange(half)[:, None] * np.arange(length)[None, :] % length) * (2.0 * np.pi / length)
    table = np.concatenate([np.cos(angle), -np.sin(angle)]) / np.sqrt(length)
    fhi = table.astype(jnp.bfloat16)
    flo = (table - fhi.astype(np.float64)).astype(jnp.bfloat16)
    vmem = pl.BlockSpec(memory_space=pltpu.VMEM)
    hbm = pl.BlockSpec(memory_space=pl.ANY)
    dma = pltpu.SemaphoreType.DMA
    return pl.pallas_call(
        functools.partial(exchange_kernel, dims, rows_y),
        out_shape=[
            jax.ShapeDtypeStruct((length * YP, CZ), jnp.float32),
            jax.ShapeDtypeStruct((2 * half * YP, CZ), jnp.float32),
        ],
        in_specs=[vmem, vmem, vmem, hbm, hbm],
        out_specs=[vmem, vmem],
        scratch_shapes=[
            pltpu.VMEM((2, band, 2 * CX), jnp.float32),
            pltpu.VMEM((2, ROWS, CZ), jnp.float32),
            pltpu.VMEM((2, ROWS, CZ), jnp.float32),
            pltpu.VMEM((groups, YP, ROWS, CZ), jnp.float32),
            pltpu.VMEM((groups, YP, ROWS, CZ), jnp.float32),
            pltpu.VMEM((2, length, YP * CZ), jnp.bfloat16),
            pltpu.VMEM((2 * half, length), jnp.bfloat16),
            pltpu.VMEM((2 * half, length), jnp.bfloat16),
            dma((2,)),
            dma((2,)),
            dma((2,)),
            dma((2,)),
            dma((2,)),
            dma((groups,)),
            dma((groups,)),
        ],
        compiler_params=pltpu.CompilerParams(collective_id=0, has_side_effects=True),
    )(core, xg, zg, jnp.asarray(fhi), jnp.asarray(flo))


def body(dims, cell_index, offsets, mass, counts):
    groups = dims[0]
    rows_y = YP * groups
    length = groups * CX
    core, xg, zg = paint(
        cell_index.reshape(1, -1), offsets.reshape(3, -1), mass.reshape(1, -1), counts.reshape(1), rows_y
    )
    density, spectrum = exchange(dims, rows_y, core, xg, zg)
    return (density.reshape(length, 1, YP, CZ), spectrum.reshape(2, length // 2, 1, YP, CZ))


def solution(mesh):
    dims = tuple(mesh.shape[axis] for axis in ("gx", "gy", "gz"))
    placed = (
        P("gx", "gy", "gz", None),
        P("gx", "gy", "gz", None, None),
        P("gx", "gy", "gz", None),
        P("gx", "gy", "gz"),
    )
    return jax.shard_map(
        functools.partial(body, dims),
        mesh=mesh,
        in_specs=placed,
        out_specs=(P(None, "gx", "gy", "gz"), P(None, None, "gx", "gy", "gz")),
        check_vma=False,
    )
```

```python
import functools
import math

import jax
import jax.numpy as jnp
import numpy as np
from jax import lax
from jax.experimental import pallas as pl
from jax.experimental.pallas import tpu as pltpu
from jax.sharding import PartitionSpec as P

MESH = pl.DeviceIdType.MESH
CX = 128
YP = 2
CZ = 128


def up(n, m):
    return -(-n // m) * m


def split(value):
    high = value.astype(jnp.bfloat16)
    low = (value - high.astype(jnp.float32)).astype(jnp.bfloat16)
    return high, low


def nt_dot(lhs, rhs):
    return lax.dot_general(lhs, rhs, (((1,), (1,)), ((), ())), preferred_element_type=jnp.float32)


def gather(full, rows):
    return (full[:rows, :128] + full[rows:, :128]) + (full[:rows, 128:] + full[rows:, 128:])


BODY = YP * CX
ROWS = BODY + 8


def paint_kernel(dims, chunk, live_ref, cell_ref, off_ref, mass_ref, out_ref, near, far, base, step_y, zrhs, lhs, accx, accz, corner, fold_x, fold_z, zin, yout, yin, pen, inbox, z_send, z_recv, y_send, y_recv, x_send, x_recv):
    groups, count_y, count_z = dims
    padded_y = YP * groups + 2
    band = up(padded_y, 8)
    stride_y = CZ + 2
    stride_x = padded_y * stride_y
    total = cell_ref.shape[1]
    pieces = total // chunk
    gx, gy, gz = lax.axis_index("gx"), lax.axis_index("gy"), lax.axis_index("gz")
    y_next = (lax.rem(gy + count_y - 1, count_y), lax.rem(gy + 1, count_y))
    z_next = (lax.rem(gz + count_z - 1, count_z), lax.rem(gz + 1, count_z))
    barrier = pltpu.get_barrier_semaphore()
    for other in z_next:
        pl.semaphore_signal(barrier, inc=1, device_id={"gz": other}, device_id_type=MESH)
    for other in y_next:
        pl.semaphore_signal(barrier, inc=1, device_id={"gy": other}, device_id_type=MESH)
    for step in range(1, groups):
        pl.semaphore_signal(barrier, inc=1, device_id={"gx": lax.rem(gx + step, groups)}, device_id_type=MESH)

    live = live_ref[0]
    accx[...] = jnp.zeros_like(accx)
    accz[...] = jnp.zeros_like(accz)
    corner[...] = jnp.zeros_like(corner)
    row_core = lax.broadcasted_iota(jnp.int32, (CX, chunk), 0).astype(jnp.float32) + 1.0
    row_band = lax.broadcasted_iota(jnp.int32, (2 * band, chunk), 0).astype(jnp.float32)

    def prepare(turn, carry):
        start = pl.multiple_of(turn * chunk, chunk)
        here = pl.ds(start, chunk)
        slot = start + lax.broadcasted_iota(jnp.int32, (1, chunk), 1)
        loaded = jnp.where(slot < live, mass_ref[:, here], 0.0)
        cell = cell_ref[:, here].astype(jnp.float32)
        x0 = jnp.floor((cell + 0.5) * (1.0 / stride_x))
        rest = cell - x0 * stride_x
        y0 = jnp.floor((rest + 0.5) * (1.0 / stride_y))
        z0 = rest - y0 * stride_y
        dx, dy, dz = off_ref[0, :, here], off_ref[1, :, here], off_ref[2, :, here]
        x1 = x0 + jnp.where(dx >= 0.0, 1.0, -1.0)
        y1 = y0 + jnp.where(dy >= 0.0, 1.0, -1.0)
        z1 = z0 + jnp.where(dz >= 0.0, 1.0, -1.0)
        fx, fy, fz = jnp.abs(dx), jnp.abs(dy), jnp.abs(dz)
        ex, ey, ez = 1.0 - fx, 1.0 - fy, 1.0 - fz
        my0, my1 = ey * loaded, fy * loaded
        base[:, here] = y0
        step_y[:, here] = y1
        zhot = jnp.where(row_core == z0, ez, jnp.where(row_core == z1, fz, 0.0))
        zhi, zlo = split(zhot)
        zboth = jnp.concatenate([zhi, zlo], axis=0)
        zrhs[turn] = zboth
        xhot = jnp.where(row_core == x0, ex, jnp.where(row_core == x1, fx, 0.0))
        xhi, xlo = split(xhot)
        near[turn] = xhot * my0
        far[turn] = xhot * my1
        yhot = jnp.where(row_band == y0, my0, jnp.where(row_band == y1, my1, 0.0)) + jnp.where(
            row_band == y0 + band, my0, jnp.where(row_band == y1 + band, my1, 0.0)
        )
        side = jnp.where(row_band >= band, 1.0, 0.0)
        ghost_x = jnp.where(x1 == side * (CX + 1.0), fx, 0.0) * yhot
        ghost_z = jnp.where(z1 == side * (CZ + 1.0), fz, 0.0) * yhot
        accx[...] += nt_dot(jnp.concatenate(split(ghost_x), axis=0), zboth)
        accz[...] += nt_dot(jnp.concatenate(split(ghost_z), axis=0), jnp.concatenate([xhi, xlo], axis=0))
        for which, edge in enumerate((0.0, CX + 1.0)):
            part = ghost_z * jnp.where(x1 == edge, fx, 0.0)
            for piece in range(chunk // 128):
                corner[which] += part[:, piece * 128 : (piece + 1) * 128]
        return carry

    lax.fori_loop(0, pieces, prepare, 0)
    fold_z[:, :CX] = gather(accz[...], 2 * band)
    lane_band = lax.broadcasted_iota(jnp.int32, (2 * band, 128), 1)
    low = jnp.sum(corner[0], axis=1, keepdims=True)
    high = jnp.sum(corner[1], axis=1, keepdims=True)
    fold_z[:, CX:] = jnp.where(lane_band == 0, low, jnp.where(lane_band == 1, high, 0.0))
    edge = gather(accx[...], 2 * band)
    pl.semaphore_wait(barrier, groups + 3)
    z_copies = [
        pltpu.make_async_remote_copy(
            src_ref=fold_z.at[pl.ds(side * band, band)],
            dst_ref=zin.at[side],
            send_sem=z_send.at[side],
            recv_sem=z_recv.at[side],
            device_id={"gz": z_next[side]},
            device_id_type=MESH,
        )
        for side in range(2)
    ]
    for copy in z_copies:
        copy.start()

    def paint_rows(first, second):
        sums = None
        for piece in range(pieces):
            here = pl.ds(piece * chunk, chunk)
            y0, y1 = base[:, here], step_y[:, here]
            for index, y in enumerate((first, second)):
                value = jnp.where(y0 == y, near[piece], jnp.where(y1 == y, far[piece], 0.0))
                high, low = split(value)
                lhs[piece % 2, pl.ds(index * 2 * CX, CX)] = high
                lhs[piece % 2, pl.ds(index * 2 * CX + CX, CX)] = low
            part = nt_dot(lhs[piece % 2], zrhs[piece])
            sums = part if sums is None else sums + part
        return gather(sums[: 2 * CX], CX), gather(sums[2 * CX :], CX)

    lane = lax.broadcasted_iota(jnp.int32, (CX, CZ), 1)
    band_row = lax.broadcasted_iota(jnp.int32, (2 * CX, band), 1)

    def fold(target, rows, indices):
        for place, (whole, index) in enumerate(zip(rows, indices)):
            for side, spot in enumerate((CZ - 1, 0)):
                column = jnp.sum(jnp.where(band_row == index, columns[side], 0.0), axis=1, keepdims=True)
                whole = whole + jnp.where(lane == spot, column[:CX], 0.0)
            target[pl.ds(place * CX, CX)] = whole
            for side in range(2):
                target[pl.ds(BODY + 2 * side + place, 1)] = fold_x[side, pl.ds(index, 1)]

    def pencil_of(turn):
        half = groups // 2
        upper = gx // half
        mine = upper * (groups - 1) + (1 - 2 * upper) * gx
        near_by = turn - (groups - half)
        near_by = near_by + jnp.where(near_by >= mine, 1, 0)
        spot = jnp.where(turn < groups - half, half + turn, jnp.where(turn == groups - 1, mine, near_by))
        return upper * (groups - 1) + (1 - 2 * upper) * spot

    def pencil_copy(target):
        return pltpu.make_async_remote_copy(
            src_ref=pen.at[target],
            dst_ref=inbox.at[gx],
            send_sem=x_send.at[target],
            recv_sem=x_recv.at[gx],
            device_id={"gx": target},
            device_id_type=MESH,
        )

    def pencil_rows(turn):
        target = pencil_of(turn)
        first = 1 + target * YP
        return target, [first + row for row in range(YP)]

    def as_float(indices):
        return [jnp.asarray(index, jnp.int32).astype(jnp.float32) for index in indices]

    start_target, start_indices = pencil_rows(0)
    start_rows = paint_rows(*as_float(start_indices))
    for copy in z_copies:
        copy.wait()
    columns = [zin[side].T for side in range(2)]
    edge_lane = lax.broadcasted_iota(jnp.int32, (band, CZ), 1)
    for x_side in range(2):
        part = edge[x_side * band : (x_side + 1) * band]
        part = part + jnp.where(edge_lane == CZ - 1, zin[0][:, CX + x_side : CX + x_side + 1], 0.0)
        fold_x[x_side] = part + jnp.where(edge_lane == 0, zin[1][:, CX + x_side : CX + x_side + 1], 0.0)
    for ref in [pen.at[t] for t in range(groups)] + [yout.at[0]]:
        ref[pl.ds(BODY, 8)] = jnp.zeros((8, CZ), jnp.float32)
    fold(pen.at[start_target], start_rows, start_indices)
    pencil_copy(start_target).start()

    ghosts = [0, padded_y - 1]
    fold(yout.at[0], paint_rows(*as_float(ghosts)), ghosts)
    y_copies = [
        pltpu.make_async_remote_copy(
            src_ref=yout.at[0, pl.ds(side * CX, CX)],
            dst_ref=yin.at[side],
            send_sem=y_send.at[side],
            recv_sem=y_recv.at[side],
            device_id={"gy": y_next[side]},
            device_id_type=MESH,
        )
        for side in range(2)
    ] + [
        pltpu.make_async_remote_copy(
            src_ref=yout.at[0, pl.ds(BODY, 8)],
            dst_ref=yin.at[2 + side, pl.ds(0, 8)],
            send_sem=y_send.at[2 + side],
            recv_sem=y_recv.at[2 + side],
            device_id={"gy": y_next[side]},
            device_id_type=MESH,
        )
        for side in range(2)
    ]
    for copy in y_copies:
        copy.start()

    def visit(turn, carry):
        target, indices = pencil_rows(turn)
        rows = paint_rows(*as_float(indices))

        @pl.when(turn == 1)
        def _():
            for copy in y_copies:
                copy.wait()

        fold(pen.at[target], rows, indices)

        @pl.when(target == 0)
        def _():
            pen[0, pl.ds(0, CX)] += yin[1]
            for side in range(2):
                pen[0, pl.ds(BODY + 2 * side, 1)] += yin[3, pl.ds(2 * side + 1, 1)]

        @pl.when(target == groups - 1)
        def _():
            pen[groups - 1, pl.ds((YP - 1) * CX, CX)] += yin[0]
            for side in range(2):
                pen[groups - 1, pl.ds(BODY + 2 * side + YP - 1, 1)] += yin[2, pl.ds(2 * side, 1)]

        @pl.when(turn < groups - 1)
        def _():
            pencil_copy(target).start()

        return carry

    lax.fori_loop(1, groups, visit, 0)
    out_ref[gx] = pen[gx]
    for step in range(1, groups):
        source = lax.rem(gx + step, groups)
        pencil_copy(source).wait_send()
        pltpu.make_async_remote_copy(
            src_ref=pen.at[source],
            dst_ref=inbox.at[source],
            send_sem=x_send.at[source],
            recv_sem=x_recv.at[source],
            device_id={"gx": source},
            device_id_type=MESH,
        ).wait_recv()
        out_ref[source] = inbox[source]


def paint(dims, cell, offs, mass, live):
    groups = dims[0]
    total = cell.shape[1]
    chunk = math.gcd(1024, total)
    band = up(YP * groups + 2, 8)
    pieces = total // chunk
    vmem = pl.BlockSpec(memory_space=pltpu.VMEM)
    dma = pltpu.SemaphoreType.DMA
    return pl.pallas_call(
        functools.partial(paint_kernel, dims, chunk),
        out_shape=jax.ShapeDtypeStruct((groups, ROWS, CZ), jnp.float32),
        in_specs=[pl.BlockSpec(memory_space=pltpu.SMEM), vmem, vmem, vmem],
        out_specs=vmem,
        scratch_shapes=[
            pltpu.VMEM((pieces, CX, chunk), jnp.float32),
            pltpu.VMEM((pieces, CX, chunk), jnp.float32),
            pltpu.VMEM((1, total), jnp.float32),
            pltpu.VMEM((1, total), jnp.float32),
            pltpu.VMEM((pieces, 2 * CZ, chunk), jnp.bfloat16),
            pltpu.VMEM((2, 2 * BODY, chunk), jnp.bfloat16),
            pltpu.VMEM((4 * band, 256), jnp.float32),
            pltpu.VMEM((4 * band, 256), jnp.float32),
            pltpu.VMEM((2, 2 * band, 128), jnp.float32),
            pltpu.VMEM((2, band, CZ), jnp.float32),
            pltpu.VMEM((2 * band, 2 * CX), jnp.float32),
            pltpu.VMEM((2, band, 2 * CX), jnp.float32),
            pltpu.VMEM((1, ROWS, CZ), jnp.float32),
            pltpu.VMEM((4, CX, CZ), jnp.float32),
            pltpu.VMEM((groups, ROWS, CZ), jnp.float32),
            pltpu.VMEM((groups, ROWS, CZ), jnp.float32),
            dma((2,)),
            dma((2,)),
            dma((4,)),
            dma((4,)),
            dma((groups,)),
            dma((groups,)),
        ],
        compiler_params=pltpu.CompilerParams(collective_id=0, has_side_effects=True),
    )(live, cell, offs, mass)


def wave_kernel(groups, in_ref, fhi, flo, dens_ref, spec_ref, flat):
    length = groups * CX
    row_id = lax.broadcasted_iota(jnp.int32, (CX, CZ), 0)
    for block in range(groups):
        before, after = (block - 1) % groups, (block + 1) % groups
        for row in range(YP):
            value = in_ref[block, row * CX : (row + 1) * CX]
            upper = BODY + 2 + row
            value = value + jnp.where(row_id == 0, in_ref[before, upper : upper + 1], 0.0)
            lower = BODY + row
            value = value + jnp.where(row_id == CX - 1, in_ref[after, lower : lower + 1], 0.0)
            dens_ref[pl.ds(block * BODY + row, CX, stride=YP), :] = value
            high, low = split(value)
            flat[0, pl.ds(block * CX, CX), pl.ds(row * CZ, CZ)] = high
            flat[1, pl.ds(block * CX, CX), pl.ds(row * CZ, CZ)] = low
    tile = 256

    def transform(turn, carry):
        start = pl.multiple_of(turn * tile, tile)
        rows = pl.ds(start, tile)
        both = jnp.dot(fhi[rows, :], flat[0], preferred_element_type=jnp.float32)
        both += jnp.dot(flo[rows, :], flat[0], preferred_element_type=jnp.float32)
        both += jnp.dot(fhi[rows, :], flat[1], preferred_element_type=jnp.float32)
        for row in range(YP):
            spec_ref[pl.ds(start * YP + row, tile, stride=YP), :] = both[:, row * CZ : (row + 1) * CZ]
        return carry

    lax.fori_loop(0, length // tile, transform, 0)


def waves(groups, pencils):
    length = groups * CX
    half = length // 2
    angle = (np.arange(half)[:, None] * np.arange(length)[None, :] % length) * (2.0 * np.pi / length)
    table = np.concatenate([np.cos(angle), -np.sin(angle)]) / np.sqrt(length)
    fhi = table.astype(jnp.bfloat16)
    flo = (table - fhi.astype(np.float64)).astype(jnp.bfloat16)
    vmem = pl.BlockSpec(memory_space=pltpu.VMEM)
    return pl.pallas_call(
        functools.partial(wave_kernel, groups),
        out_shape=[
            jax.ShapeDtypeStruct((length * YP, CZ), jnp.float32),
            jax.ShapeDtypeStruct((2 * half * YP, CZ), jnp.float32),
        ],
        in_specs=[vmem] * 3,
        out_specs=[vmem] * 2,
        scratch_shapes=[pltpu.VMEM((2, length, YP * CZ), jnp.bfloat16)],
    )(pencils, jnp.asarray(fhi), jnp.asarray(flo))


def body(dims, cell_index, offsets, mass, counts):
    length = dims[0] * CX
    pencils = paint(
        dims, cell_index.reshape(1, -1), offsets.reshape(3, 1, -1), mass.reshape(1, -1), counts.reshape(1)
    )
    density, spectrum = waves(dims[0], pencils)
    return (density.reshape(length, 1, YP, CZ), spectrum.reshape(2, length // 2, 1, YP, CZ))


def solution(mesh):
    dims = tuple(mesh.shape[axis] for axis in ("gx", "gy", "gz"))
    placed = (
        P("gx", "gy", "gz", None),
        P("gx", "gy", "gz", None, None),
        P("gx", "gy", "gz", None),
        P("gx", "gy", "gz"),
    )
    return jax.shard_map(
        functools.partial(body, dims),
        mesh=mesh,
        in_specs=placed,
        out_specs=(P(None, "gx", "gy", "gz"), P(None, None, "gx", "gy", "gz")),
        check_vma=False,
    )
```
